8 devices in a mesh: data: 2 (over z, y), tp: 4 (over x, core).
Axes of the slice: x: 2, y: 2, z: 1, core: 2. Of those that a mesh axis runs over, the one named last changes fastest.
Arguments:
- x_all: bfloat16 [256, 4096], P(('data', 'tp')), parts along dimension 0
- ln_gammas: float32 [2, 4096], replicated
- w_in: bfloat16 [2, 4096, 16384], P(None, None, 'tp')
- w_out: bfloat16 [2, 16384, 4096], P(None, 'tp')
Outputs:
- output: bfloat16 [256, 4096], P(('data', 'tp')), parts along dimension 0
There are 2 independent parts. The reference program is written for one: setup_inputs(seed, part) draws one part's arguments, and reference() takes and returns one part's arrays. A program takes and returns all parts, laid end to end along the dimension named above; an argument that names none is the same for every part.
All inputs are finite; a program needn't handle non-finite values.
Results may differ from the reference program's by a relative error of at most 0.0100171.
Values are sent between devices in bfloat16 or wider.
A program may use at most 1 GiB of HBM per device.

```python
import math
import jax
import jax.numpy as jnp
from jax import lax

SEQ_LEN = 128
D_MODEL = 4096
FF_WIDTH = 16384
NUM_LAYERS = 2

LN_EPS = 1e-6
ROW_BLOCK = math.gcd(SEQ_LEN, 512)


def setup_inputs(seed: int = 0, part: int = 0) -> dict:
    part_key = jax.random.fold_in(jax.random.key(seed), part)
    shared_key = jax.random.key(seed + 1)
    key_gamma, key_in, key_out = jax.random.split(shared_key, 3)
    x_all = jax.random.normal(part_key, (SEQ_LEN, D_MODEL), jnp.float32).astype(jnp.bfloat16)
    ln_gammas = 1.0 + 0.25 * jax.random.normal(key_gamma, (NUM_LAYERS, D_MODEL), jnp.float32)
    w_in = (jax.random.normal(key_in, (NUM_LAYERS, D_MODEL, FF_WIDTH), jnp.float32) * D_MODEL ** -0.5).astype(jnp.bfloat16)
    w_out = (jax.random.normal(key_out, (NUM_LAYERS, FF_WIDTH, D_MODEL), jnp.float32) * (1.5 * FF_WIDTH ** -0.5)).astype(jnp.bfloat16)
    return {"x_all": x_all, "ln_gammas": ln_gammas, "w_in": w_in, "w_out": w_out}


def mlp_layer(x_rows, gamma_row, w_in_layer, w_out_layer):
    x_f32 = x_rows.astype(jnp.float32)
    mean_val = jnp.mean(x_f32, axis=-1, keepdims=True)
    centered = x_f32 - mean_val
    var_val = jnp.mean(centered * centered, axis=-1, keepdims=True)
    normed = (centered * lax.rsqrt(var_val + LN_EPS) * gamma_row).astype(jnp.bfloat16)
    hidden = jax.nn.gelu(jnp.dot(normed, w_in_layer, preferred_element_type=jnp.float32), approximate=True).astype(jnp.bfloat16)
    mlp_out = jnp.dot(hidden, w_out_layer, preferred_element_type=jnp.float32)
    return (x_f32 + mlp_out).astype(jnp.bfloat16)


def reference(x_all, ln_gammas, w_in, w_out):
    row_blocks = x_all.reshape(SEQ_LEN // ROW_BLOCK, ROW_BLOCK, D_MODEL)

    def run_block(rows):
        def layer_step(carry, layer_params):
            gamma_row, w_in_layer, w_out_layer = layer_params
            return mlp_layer(carry, gamma_row, w_in_layer, w_out_layer), None
        final_rows, _ = lax.scan(layer_step, rows, (ln_gammas, w_in, w_out))
        return final_rows

    return lax.map(run_block, row_blocks).reshape(SEQ_LEN, D_MODEL)
```

```python
import functools

import jax
import jax.numpy as jnp
from jax import lax
from jax.experimental import pallas as pl
from jax.experimental.pallas import tpu as pltpu
from jax.sharding import PartitionSpec as P

LN_EPS = 1e-6
CHUNK = 512
W2_SLOTS = 5
MESH = pl.DeviceIdType.MESH
F32 = jnp.float32
BF16 = jnp.bfloat16


def gelu_tanh(u):
    c = 0.7978845608028654
    return 0.5 * u * (1.0 + jnp.tanh(c * (u + 0.044715 * (u * u * u))))


def mlp_kernel(
    x_hbm, g_hbm, w1_hbm, w2_hbm, out_hbm,
    res, gv, w1s, w2s, xn, u, h, pb, rb, sb, xr,
    in_sem, w1_sem, w2_sem, out_sem,
    agp_s, agp_r, agx_s, agx_r, agr_s, agr_r, dd_s, dd_r, lk_s, lk_r,
):
    layers, d_model, ff = w1_hbm.shape
    rows = x_hbm.shape[0]
    nc = d_model // CHUNK
    data_i = lax.axis_index("data")
    me = lax.axis_index("tp")
    core = lax.rem(me, 2)
    chip = lax.div(me, 2)
    partner = me + 1 - 2 * core
    xpeer = me + 2 - 4 * chip

    def w1_copy(l, k):
        return pltpu.make_async_copy(
            w1_hbm.at[l, pl.ds(pl.multiple_of(k * CHUNK, CHUNK), CHUNK), :], w1s.at[k], w1_sem.at[k])

    def w2_copy(l, n):
        slot = lax.rem(n + l * nc, W2_SLOTS)
        return pltpu.make_async_copy(
            w2_hbm.at[l, :, pl.ds(pl.multiple_of(n * CHUNK, CHUNK), CHUNK)], w2s.at[slot], w2_sem.at[slot])

    def remote(src, dst, ssem, rsem, to):
        return pltpu.make_async_remote_copy(
            src_ref=src, dst_ref=dst, send_sem=ssem, recv_sem=rsem,
            device_id=(data_i, to), device_id_type=MESH)

    def ag_partner(l, k):
        return remote(xn.at[k, me], xn.at[k, me], agp_s.at[l, k], agp_r.at[l, k], partner)

    def ag_x(l, k):
        return remote(xn.at[k, me], xn.at[k, me], agx_s.at[l, k], agx_r.at[l, k], xpeer)

    def ag_relay(l, k):
        return remote(xn.at[k, xpeer], xn.at[k, xpeer], agr_s.at[l, k], agr_r.at[l, k], partner)

    def rs_partner(l, n):
        return remote(pb.at[n, 1 - core], rb.at[n], dd_s.at[l, n], dd_r.at[l, n], partner)

    def rs_x(l, n):
        return remote(sb.at[n, 1 - chip], xr.at[n], lk_s.at[l, n], lk_r.at[l, n], xpeer)

    x_in = pltpu.make_async_copy(x_hbm, res, in_sem.at[0])
    g_in = pltpu.make_async_copy(g_hbm, gv, in_sem.at[1])
    x_in.start()
    g_in.start()
    for k in range(nc):
        w1_copy(0, k).start()
    for n in range(W2_SLOTS):
        w2_copy(0, n).start()

    barrier = pltpu.get_barrier_semaphore()
    for peer in (partner, xpeer):
        pl.semaphore_signal(barrier, inc=1, device_id=(data_i, peer), device_id_type=MESH)
    x_in.wait()
    g_in.wait()
    pl.semaphore_wait(barrier, 2)

    def cols(n):
        return pl.ds(n * CHUNK, CHUNK)

    for l in range(layers):
        total = res[:, cols(0)].astype(F32)
        for n in range(1, nc):
            total += res[:, cols(n)].astype(F32)
        mean = jnp.sum(total, axis=-1, keepdims=True) * (1.0 / d_model)
        total = None
        for n in range(nc):
            cen = res[:, cols(n)].astype(F32) - mean
            total = cen * cen if total is None else total + cen * cen
        var = jnp.sum(total, axis=-1, keepdims=True) * (1.0 / d_model)
        inv = lax.rsqrt(var + LN_EPS)
        for k in range(nc):
            cen = res[:, cols(k)].astype(F32) - mean
            xn[k, me] = (cen * inv * gv[pl.ds(l, 1), cols(k)]).astype(BF16)
            ag_x(l, k).start()
            ag_partner(l, k).start()

        def arrive(k):
            ag_x(l, k).wait_recv()
            ag_relay(l, k).start()

        def ready(k):
            ag_partner(l, k).wait_recv()
            ag_relay(l, k).wait_recv()
            w1_copy(l, k).wait()

        def w1_block(k, n):
            lhs = xn[k].reshape(4 * rows, CHUNK)
            return jnp.dot(lhs, w1s[k, :, cols(n)], preferred_element_type=F32)

        arrive(0)
        arrive(1)
        ready(0)
        for n in range(ff // CHUNK):
            u[:, cols(n)] = w1_block(0, n)

        @pl.loop(1, nc - 1)
        def _(k):
            arrive(k + 1)
            ready(k)
            for n in range(ff // CHUNK):
                u[:, cols(n)] += w1_block(k, n)

        ready(nc - 1)
        for n in range(ff // CHUNK):
            h[:, cols(n)] = gelu_tanh(u[:, cols(n)] + w1_block(nc - 1, n)).astype(BF16)

        for k in range(nc):
            ag_x(l, k).wait_send()
            ag_partner(l, k).wait_send()
            ag_relay(l, k).wait_send()

        def finish(n):
            rs_partner(l, n).wait()
            sb[n] = pb[n, core] + rb[n]
            rs_x(l, n).start()

        @pl.loop(0, nc)
        def _(n):
            w2_copy(l, n).wait()
            slot = lax.rem(n + l * nc, W2_SLOTS)
            acc = jnp.dot(h[...], w2s[slot], preferred_element_type=F32)
            for d in range(4):
                pb[n, d % 2, d // 2] = acc[d * rows:(d + 1) * rows]
            rs_partner(l, n).start()

            @pl.when(n + W2_SLOTS < nc)
            def _():
                w2_copy(l, n + W2_SLOTS).start()

            if l + 1 < layers:
                @pl.when(n + W2_SLOTS >= nc)
                def _():
                    w1_copy(l + 1, n + W2_SLOTS - nc).start()

            @pl.when(n > 0)
            def _():
                finish(n - 1)

        if l + 1 < layers:
            for k in range(W2_SLOTS, nc):
                w1_copy(l + 1, k).start()
            for n in range(W2_SLOTS):
                w2_copy(l + 1, n).start()
        finish(nc - 1)

        outs = []
        for n in range(nc):
            rs_x(l, n).wait()
            y = res[:, cols(n)].astype(F32) + (sb[n, chip] + xr[n])
            res[:, cols(n)] = y.astype(BF16)
            if l + 1 == layers:
                out = pltpu.make_async_copy(res.at[:, cols(n)], out_hbm.at[:, cols(n)], out_sem.at[n])
                out.start()
                outs.append(out)
        for out in outs:
            out.wait()


def solution(mesh):
    def local_stack(x_local, ln_gammas, w_in, w_out):
        rows, d_model = x_local.shape
        layers, _, ff = w_in.shape
        nc = d_model // CHUNK
        dma = pltpu.SemaphoreType.DMA
        pair = [dma((layers, nc)), dma((layers, nc))]
        return pl.pallas_call(
            mlp_kernel,
            out_shape=jax.ShapeDtypeStruct((rows, d_model), BF16),
            in_specs=[pl.BlockSpec(memory_space=pl.ANY)] * 4,
            out_specs=pl.BlockSpec(memory_space=pl.ANY),
            scratch_shapes=[
                pltpu.VMEM((rows, d_model), BF16),
                pltpu.VMEM(ln_gammas.shape, F32),
                pltpu.VMEM((nc, CHUNK, ff), BF16),
                pltpu.VMEM((W2_SLOTS, ff, CHUNK), BF16),
                pltpu.VMEM((nc, 4, rows, CHUNK), BF16),
                pltpu.VMEM((4 * rows, ff), F32),
                pltpu.VMEM((4 * rows, ff), BF16),
                pltpu.VMEM((nc, 2, 2, rows, CHUNK), F32),
                pltpu.VMEM((nc, 2, rows, CHUNK), F32),
                pltpu.VMEM((nc, 2, rows, CHUNK), F32),
                pltpu.VMEM((nc, rows, CHUNK), F32),
                dma((2,)), dma((nc,)), dma((W2_SLOTS,)), dma((nc,)),
            ] + pair * 5,
            compiler_params=pltpu.CompilerParams(
                collective_id=0, has_side_effects=True, vmem_limit_bytes=67043328),
            name="mlp_stack",
        )(x_local, ln_gammas, w_in, w_out)

    return jax.shard_map(
        local_stack,
        mesh=mesh,
        in_specs=(P(('data', 'tp'), None), P(None, None), P(None, None, 'tp'), P(None, 'tp', None)),
        out_specs=P(('data', 'tp'), None),
        check_vma=False,
    )
```

```python
import functools

import jax
import jax.numpy as jnp
from jax import lax
from jax.experimental import pallas as pl
from jax.experimental.pallas import tpu as pltpu
from jax.sharding import PartitionSpec as P

LN_EPS = 1e-6
CHUNK = 512
PART = 256
W2_SLOTS = 5
MESH = pl.DeviceIdType.MESH
F32 = jnp.float32
BF16 = jnp.bfloat16


def gelu_tanh(u):
    c = 0.7978845608028654
    return 0.5 * u * (1.0 + jnp.tanh(c * (u + 0.044715 * (u * u * u))))


def mlp_kernel(
    x_hbm, g_hbm, w1_hbm, w2_hbm, out_ref,
    res, gv, w1s, w2s, xn, u, h, pb, rb, sb, xr,
    in_sem, w1_sem, w2_sem,
    agp_s, agp_r, agx_s, agx_r, agr_s, agr_r, dd_s, dd_r, lk_s, lk_r,
):
    layers, d_model, ff = w1_hbm.shape
    rows = x_hbm.shape[0]
    nc = d_model // CHUNK
    halves = CHUNK // PART
    data_i = lax.axis_index("data")
    me = lax.axis_index("tp")
    core = lax.rem(me, 2)
    chip = lax.div(me, 2)
    partner = me + 1 - 2 * core
    xpeer = me + 2 - 4 * chip

    def w1_copy(l, k):
        return pltpu.make_async_copy(
            w1_hbm.at[l, pl.ds(pl.multiple_of(k * CHUNK, CHUNK), CHUNK), :], w1s.at[k], w1_sem.at[k])

    def w2_copy(l, n):
        slot = lax.rem(n + l * nc, W2_SLOTS)
        return pltpu.make_async_copy(
            w2_hbm.at[l, :, pl.ds(pl.multiple_of(n * CHUNK, CHUNK), CHUNK)], w2s.at[slot], w2_sem.at[slot])

    def remote(src, dst, ssem, rsem, to):
        return pltpu.make_async_remote_copy(
            src_ref=src, dst_ref=dst, send_sem=ssem, recv_sem=rsem,
            device_id=(data_i, to), device_id_type=MESH)

    def ag_partner(k):
        return remote(xn.at[k, me], xn.at[k, me], agp_s.at[0], agp_r.at[k], partner)

    def ag_x(k):
        return remote(xn.at[k, me], xn.at[k, me], agx_s.at[0], agx_r.at[k], xpeer)

    def ag_relay(k):
        return remote(xn.at[k, xpeer], xn.at[k, xpeer], agr_s.at[0], agr_r.at[k], partner)

    def rs_partner(j):
        return remote(pb.at[j, 1 - core], rb.at[j], dd_s.at[0], dd_r.at[j], partner)

    def rs_x(j):
        return remote(sb.at[j, 1 - chip], xr.at[j], lk_s.at[0], lk_r.at[j], xpeer)

    x_in = pltpu.make_async_copy(x_hbm, res, in_sem.at[0])
    g_in = pltpu.make_async_copy(g_hbm, gv, in_sem.at[1])
    x_in.start()
    g_in.start()
    w1_copy(0, nc - 1).start(priority=1)
    barrier = pltpu.get_barrier_semaphore()
    for peer in (partner, xpeer):
        pl.semaphore_signal(barrier, inc=1, device_id=(data_i, peer), device_id_type=MESH)
    x_in.wait()
    g_in.wait()
    for k in range(nc - 1):
        w1_copy(0, k).start()
    for n in range(W2_SLOTS):
        w2_copy(0, n).start(priority=1)

    def cols(n, width=CHUNK):
        return pl.ds(n * width, width)

    total = None
    for n in range(nc):
        y = res[:, cols(n)].astype(F32)
        total = y if total is None else total + y

    for l in range(layers):
        mean = jnp.sum(total, axis=-1, keepdims=True) * (1.0 / d_model)
        total = None
        for n in range(nc):
            cen = res[:, cols(n)].astype(F32) - mean
            total = cen * cen if total is None else total + cen * cen
        var = jnp.sum(total, axis=-1, keepdims=True) * (1.0 / d_model)
        inv = lax.rsqrt(var + LN_EPS)
        if l == 0:
            pl.semaphore_wait(barrier, 2)
        for k in range(nc):
            cen = res[:, cols(k)].astype(F32) - mean
            xn[k, me] = (cen * inv * gv[pl.ds(l, 1), cols(k)]).astype(BF16)
            ag_x(k).start()
            ag_partner(k).start()

        def arrive(k):
            ag_x(k).wait_recv()
            ag_relay(k).start()

        def ready(k):
            ag_partner(k).wait_recv()
            ag_relay(k).wait_recv()
            w1_copy(l, k).wait()

        def w1_block(k, n):
            lhs = xn[k].reshape(4 * rows, CHUNK)
            return jnp.dot(lhs, w1s[k, :, cols(n)], preferred_element_type=F32)

        arrive(0)
        arrive(1)
        ready(0)
        for n in range(ff // CHUNK):
            u[:, cols(n)] = w1_block(0, n)

        @pl.loop(1, nc - 1)
        def _(k):
            arrive(k + 1)
            ready(k)
            for n in range(ff // CHUNK):
                u[:, cols(n)] += w1_block(k, n)

        ready(nc - 1)
        for n in range(ff // CHUNK):
            h[:, cols(n)] = gelu_tanh(u[:, cols(n)] + w1_block(nc - 1, n)).astype(BF16)

        remote(xn.at[:, me], xn.at[:, me], agx_s.at[0], agx_r.at[0], xpeer).wait_send()
        remote(xn.at[:, me], xn.at[:, me], agp_s.at[0], agp_r.at[0], partner).wait_send()
        remote(xn.at[:, me], xn.at[:, me], agr_s.at[0], agr_r.at[0], partner).wait_send()

        def finish(j):
            rs_partner(j).wait_recv()
            sb[j] = pb[j, core] + rb[j]
            rs_x(j).start()

        @pl.loop(0, nc)
        def _(n):
            w2_copy(l, n).wait()
            slot = lax.rem(n + l * nc, W2_SLOTS)
            acc = jnp.dot(h[...], w2s[slot], preferred_element_type=F32)
            for s in range(halves):
                for d in range(4):
                    pb[n * halves + s, d % 2, d // 2] = acc[d * rows:(d + 1) * rows, s * PART:(s + 1) * PART]
                rs_partner(n * halves + s).start()

            @pl.when(n > 0)
            def _():
                for s in range(halves):
                    finish((n - 1) * halves + s)

            @pl.when(n + W2_SLOTS < nc)
            def _():
                w2_copy(l, n + W2_SLOTS).start(priority=1)

            if l + 1 < layers:
                @pl.when(n + W2_SLOTS >= nc)
                def _():
                    w1_copy(l + 1, n + W2_SLOTS - nc).start(priority=1)

        if l + 1 < layers:
            for k in range(W2_SLOTS, nc):
                w1_copy(l + 1, k).start()
            for n in range(W2_SLOTS):
                w2_copy(l + 1, n).start(priority=1)
        for s in range(halves):
            finish((nc - 1) * halves + s)

        remote(pb.at[:, 0], rb, dd_s.at[0], dd_r.at[0], partner).wait_send()

        total = None
        for j in range(nc * halves):
            rs_x(j).wait_recv()
            y = res[:, cols(j, PART)].astype(F32) + (sb[j, chip] + xr[j])
            y = y.astype(BF16)
            res[:, cols(j, PART)] = y
            y = y.astype(F32)
            total = y if total is None else total + y
        remote(sb.at[:, 0], xr, lk_s.at[0], lk_r.at[0], xpeer).wait_send()
    out_ref[...] = res[...]


def solution(mesh):
    def local_stack(x_local, ln_gammas, w_in, w_out):
        rows, d_model = x_local.shape
        layers, _, ff = w_in.shape
        nc = d_model // CHUNK
        dma = pltpu.SemaphoreType.DMA
        parts = d_model // PART
        return pl.pallas_call(
            mlp_kernel,
            out_shape=pltpu.VMEM((rows, d_model), BF16),
            in_specs=[pl.BlockSpec(memory_space=pl.ANY)] * 4,
            out_specs=pl.BlockSpec(memory_space=pltpu.VMEM),
            scratch_shapes=[
                pltpu.VMEM((rows, d_model), BF16),
                pltpu.VMEM(ln_gammas.shape, F32),
                pltpu.VMEM((nc, CHUNK, ff), BF16),
                pltpu.VMEM((W2_SLOTS, ff, CHUNK), BF16),
                pltpu.VMEM((nc, 4, rows, CHUNK), BF16),
                pltpu.VMEM((4 * rows, ff), F32),
                pltpu.VMEM((4 * rows, ff), BF16),
                pltpu.VMEM((parts, 2, 2, rows, PART), F32),
                pltpu.VMEM((parts, 2, rows, PART), F32),
                pltpu.VMEM((parts, 2, rows, PART), F32),
                pltpu.VMEM((parts, rows, PART), F32),
                dma((2,)), dma((nc,)), dma((W2_SLOTS,)),
                dma((1,)), dma((nc,)), dma((1,)), dma((nc,)), dma((1,)), dma((nc,)),
                dma((1,)), dma((parts,)), dma((1,)), dma((parts,)),
            ],
            compiler_params=pltpu.CompilerParams(
                collective_id=0, has_side_effects=True, vmem_limit_bytes=65536000),
            name="mlp_stack",
        )(x_local, ln_gammas, w_in, w_out)

    return jax.shard_map(
        local_stack,
        mesh=mesh,
        in_specs=(P(('data', 'tp'), None), P(None, None), P(None, None, 'tp'), P(None, 'tp', None)),
        out_specs=P(('data', 'tp'), None),
        check_vma=False,
    )
```

```python
import functools

import jax
import jax.numpy as jnp
from jax import lax
from jax.experimental import pallas as pl
from jax.experimental.pallas import tpu as pltpu
from jax.sharding import PartitionSpec as P

LN_EPS = 1e-6
CHUNK = 512
PART = 256
W2_SLOTS = 5
MESH = pl.DeviceIdType.MESH
F32 = jnp.float32
BF16 = jnp.bfloat16


def gelu_tanh(u):
    c = 0.7978845608028654
    return (0.5 * u) * (1.0 + jnp.tanh(u * (c + (c * 0.044715) * (u * u))))


def mlp_kernel(
    x_hbm, g_hbm, w1_hbm, w2_hbm, out_ref,
    res, gv, w1s, w2s, xn, u, h, pb, rb, sb, xr,
    in_sem, w1_sem, w2_sem,
    agp_s, agp_r, agx_s, agx_r, agr_s, agr_r, dd_s, dd_r, lk_s, lk_r,
):
    layers, d_model, ff = w1_hbm.shape
    rows = x_hbm.shape[0]
    nc = d_model // CHUNK
    halves = CHUNK // PART
    data_i = lax.axis_index("data")
    me = lax.axis_index("tp")
    core = lax.rem(me, 2)
    chip = lax.div(me, 2)
    partner = me + 1 - 2 * core
    xpeer = me + 2 - 4 * chip

    def cols(n, width=CHUNK):
        return pl.ds(n * width, width)

    def w1_copy(l, k):
        return pltpu.make_async_copy(
            w1_hbm.at[l, pl.ds(pl.multiple_of(k * CHUNK, CHUNK), CHUNK), :], w1s.at[k], w1_sem.at[k])

    def w2_copy(l, n):
        slot = lax.rem(n + l * nc, W2_SLOTS)
        return pltpu.make_async_copy(
            w2_hbm.at[l, :, pl.ds(pl.multiple_of(n * CHUNK, CHUNK), CHUNK)], w2s.at[slot], w2_sem.at[slot])

    def remote(src, dst, ssem, rsem, to):
        return pltpu.make_async_remote_copy(
            src_ref=src, dst_ref=dst, send_sem=ssem, recv_sem=rsem,
            device_id=(data_i, to), device_id_type=MESH)

    def ag_partner(k):
        return remote(xn.at[k, me], xn.at[k, me], agp_s.at[0], agp_r.at[k], partner)

    def ag_x(k):
        return remote(xn.at[k, me], xn.at[k, me], agx_s.at[0], agx_r.at[k], xpeer)

    def ag_relay(k):
        return remote(xn.at[k, xpeer], xn.at[k, xpeer], agr_s.at[0], agr_r.at[k], partner)

    def rs_partner(j):
        return remote(pb.at[j, 1 - core], rb.at[j], dd_s.at[0], dd_r.at[j], partner)

    def rs_x(j):
        return remote(sb.at[j, 1 - chip], xr.at[j], lk_s.at[0], lk_r.at[j], xpeer)

    x_in = pltpu.make_async_copy(x_hbm, res, in_sem.at[0])
    g_in = pltpu.make_async_copy(g_hbm, gv, in_sem.at[1])
    x_in.start()
    g_in.start()
    w1_copy(0, 0).start(priority=1)
    barrier = pltpu.get_barrier_semaphore()
    for peer in (partner, xpeer):
        pl.semaphore_signal(barrier, inc=1, device_id=(data_i, peer), device_id_type=MESH)
    x_in.wait()
    g_in.wait()
    for k in range(1, nc):
        w1_copy(0, k).start()
    for n in range(W2_SLOTS):
        w2_copy(0, n).start(priority=1)

    total = None
    for n in range(nc):
        y = res[:, cols(n)].astype(F32)
        total = y if total is None else total + y

    for l in range(layers):
        mean = jnp.sum(total, axis=-1, keepdims=True) * (1.0 / d_model)
        total = None
        for n in range(nc):
            cen = res[:, cols(n)].astype(F32) - mean
            total = cen * cen if total is None else total + cen * cen
        var = jnp.sum(total, axis=-1, keepdims=True) * (1.0 / d_model)
        inv = lax.rsqrt(var + LN_EPS)
        if l == 0:
            pl.semaphore_wait(barrier, 2)
        for k in range(nc):
            cen = res[:, cols(k)].astype(F32) - mean
            xn[k, me] = (cen * inv * gv[pl.ds(l, 1), cols(k)]).astype(BF16)
            ag_x(k).start()
            ag_partner(k).start()

        def arrive(k):
            ag_x(k).wait_recv()
            ag_relay(k).start()

        def ready(k):
            ag_partner(k).wait_recv()
            ag_relay(k).wait_recv()
            w1_copy(l, k).wait()

        def w1_block(k, n):
            lhs = xn[k].reshape(4 * rows, CHUNK)
            return jnp.dot(lhs, w1s[k, :, cols(n)], preferred_element_type=F32)

        arrive(0)
        arrive(1)
        ready(0)
        for n in range(ff // CHUNK):
            u[:, cols(n)] = w1_block(0, n)

        @pl.loop(1, nc - 1)
        def _(k):
            arrive(k + 1)
            ready(k)
            for n in range(ff // CHUNK):
                u[:, cols(n)] += w1_block(k, n)

        def finish(j):
            rs_partner(j).wait_recv()
            sb[j] = pb[j, core] + rb[j]
            rs_x(j).start()

        def partial_sums(n, slot):
            send_partial(n, jnp.dot(h[...], w2s[slot], preferred_element_type=F32))

        def send_partial(n, acc):
            for s in range(halves):
                send_part(n * halves + s, acc[:, s * PART:(s + 1) * PART])

        def send_part(j, acc):
            for d in range(4):
                pb[j, d % 2, d // 2] = acc[d * rows:(d + 1) * rows]
            rs_partner(j).start()

        def refill(n):
            @pl.when(n + W2_SLOTS < nc)
            def _():
                w2_copy(l, n + W2_SLOTS).start(priority=1)

            if l + 1 < layers:
                @pl.when(n + W2_SLOTS >= nc)
                def _():
                    w1_copy(l + 1, n + W2_SLOTS - nc).start(priority=1)

        slot = (l * nc) % W2_SLOTS
        ready(nc - 1)
        if l == 0:
            for n in range(ff // CHUNK):
                h[:, cols(n)] = gelu_tanh(u[:, cols(n)] + w1_block(nc - 1, n)).astype(BF16)
            w2_copy(l, 0).wait()
            acc = jnp.dot(h[...], w2s[slot], preferred_element_type=F32)
        else:
            w2_copy(l, 0).wait()
            acc, ahead = None, None
            for n in range(ff // CHUNK + 1):
                here = None
                if n < ff // CHUNK:
                    here = gelu_tanh(u[:, cols(n)] + w1_block(nc - 1, n)).astype(BF16)
                    h[:, cols(n)] = here
                if n > 0:
                    part = jnp.dot(ahead, w2s[slot, cols(n - 1), :], preferred_element_type=F32)
                    acc = part if acc is None else acc + part
                ahead = here
        send_partial(0, acc)
        refill(0)

        remote(xn.at[:, me], xn.at[:, me], agx_s.at[0], agx_r.at[0], xpeer).wait_send()
        remote(xn.at[:, me], xn.at[:, me], agp_s.at[0], agp_r.at[0], partner).wait_send()
        remote(xn.at[:, me], xn.at[:, me], agr_s.at[0], agr_r.at[0], partner).wait_send()

        @pl.loop(1, nc)
        def _(n):
            w2_copy(l, n).wait()
            partial_sums(n, lax.rem(n + l * nc, W2_SLOTS))
            refill(n)

            for s in range(halves):
                finish((n - 1) * halves + s)

        if l + 1 < layers:
            for k in range(W2_SLOTS, nc):
                w1_copy(l + 1, k).start()
            for n in range(W2_SLOTS):
                w2_copy(l + 1, n).start(priority=1)
        for s in range(halves):
            finish((nc - 1) * halves + s)

        remote(pb.at[:, 0], rb, dd_s.at[0], dd_r.at[0], partner).wait_send()

        total = None
        for j in range(nc * halves):
            rs_x(j).wait_recv()
            y = res[:, cols(j, PART)].astype(F32) + (sb[j, chip] + xr[j])
            y = y.astype(BF16)
            res[:, cols(j, PART)] = y
            y = y.astype(F32)
            total = y if total is None else total + y
        remote(sb.at[:, 0], xr, lk_s.at[0], lk_r.at[0], xpeer).wait_send()
    out_ref[...] = res[...]


def solution(mesh):
    def local_stack(x_local, ln_gammas, w_in, w_out):
        rows, d_model = x_local.shape
        layers, _, ff = w_in.shape
        nc = d_model // CHUNK
        dma = pltpu.SemaphoreType.DMA
        parts = d_model // PART
        return pl.pallas_call(
            mlp_kernel,
            out_shape=pltpu.VMEM((rows, d_model), BF16),
            in_specs=[pl.BlockSpec(memory_space=pl.ANY)] * 4,
            out_specs=pl.BlockSpec(memory_space=pltpu.VMEM),
            scratch_shapes=[
                pltpu.VMEM((rows, d_model), BF16),
                pltpu.VMEM(ln_gammas.shape, F32),
                pltpu.VMEM((nc, CHUNK, ff), BF16),
                pltpu.VMEM((W2_SLOTS, ff, CHUNK), BF16),
                pltpu.VMEM((nc, 4, rows, CHUNK), BF16),
                pltpu.VMEM((4 * rows, ff), F32),
                pltpu.VMEM((4 * rows, ff), BF16),
                pltpu.VMEM((parts, 2, 2, rows, PART), F32),
                pltpu.VMEM((parts, 2, rows, PART), F32),
                pltpu.VMEM((parts, 2, rows, PART), F32),
                pltpu.VMEM((parts, rows, PART), F32),
                dma((2,)), dma((nc,)), dma((W2_SLOTS,)),
                dma((1,)), dma((nc,)), dma((1,)), dma((nc,)), dma((1,)), dma((nc,)),
                dma((1,)), dma((parts,)), dma((1,)), dma((parts,)),
            ],
            compiler_params=pltpu.CompilerParams(
                collective_id=0, has_side_effects=True, vmem_limit_bytes=65536000),
            name="mlp_stack",
        )(x_local, ln_gammas, w_in, w_out)

    return jax.shard_map(
        local_stack,
        mesh=mesh,
        in_specs=(P(('data', 'tp'), None), P(None, None), P(None, None, 'tp'), P(None, 'tp', None)),
        out_specs=P(('data', 'tp'), None),
        check_vma=False,
    )
```
